768 devices in a mesh: row: 12 (over z), col: 64 (over y, x, core).
Axes of the slice: x: 4, y: 8, z: 12, core: 2. Of those that a mesh axis runs over, the one named last changes fastest.
Arguments:
- positions: float32 [3, 12582912], P(None, ('row', 'col')), may hold values from 0 to 1
- masses: float32 [1, 12582912], P(None, ('row', 'col')), may hold values from 2e-09 to 2e-08
- counts: int32 [1, 98304], P(None, ('row', 'col')), may hold values from 32 to 128
- sources: int32 [98304, 8], P(('row', 'col')), may hold values from 0 to 383, as said below
Outputs:
- accel: float32 [3, 12582912], P(None, ('row', 'col'))
The draws below stay inside these ranges and needn't reach their ends.
Inputs may be any that keep to these rules, and one draw needn't show every extreme that they name: `sources`: each device's source ids name exactly 32 distinct leaves of the lower row neighbour and exactly 32 of the upper one.
All inputs are finite; a program needn't handle non-finite values.
Results may differ from the reference program's by a relative error of at most 0.00024.
Values sent between devices are 32-bit elements; how exact they have to be, the bound alone decides.
No kernel may reach another device: no remote copies, remote signals or barrier semaphores. Data moves between devices by JAX's collectives and lax.ppermute only.
A program may use at most 32 MiB of HBM per device.

```python
import math
import jax
import jax.numpy as jnp
from jax import lax

LEAF = 128
K = 8
BLK = 2
NL = 128
REQ = 32
ROWS = 12582912
N_ROW = 12
N_COL = 64
DEVICES = 768


cell_width = 0.0025


def draw_sources(key, part):

    def one_device(device):
        sub = jax.random.fold_in(jax.random.fold_in(key, 7011), device)
        key_low, key_high, key_rest, key_perm = jax.random.split(sub, 4)
        low_pick = jax.random.permutation(key_low, NL)[:REQ].astype(jnp.int32) + NL
        high_pick = jax.random.permutation(key_high, NL)[:REQ].astype(jnp.int32) + 2 * NL
        candidates = jnp.concatenate([jnp.arange(NL, dtype=jnp.int32), low_pick, high_pick])
        chosen = jax.random.randint(key_rest, (NL * K - 2 * REQ,), 0, NL + 2 * REQ)
        listed = jnp.concatenate([low_pick, high_pick, candidates[chosen]])
        order = jax.random.permutation(key_perm, NL * K)
        return listed[order].reshape(NL, K)
    return jax.vmap(one_device)(jnp.arange(DEVICES, dtype=jnp.int32)).reshape(DEVICES * NL, K)


def draw_positions(key, part):
    sub = jax.random.fold_in(key, 5123)
    key_leaf, key_slot = jax.random.split(sub, 2)
    index = jnp.arange(ROWS, dtype=jnp.int32)
    per_device = NL * LEAF
    sender = index // per_device
    row_index = (sender // N_COL).astype(jnp.float32)
    target_col = (index % per_device // (BLK * LEAF)).astype(jnp.float32)
    leaf_index = index // LEAF
    radius = N_ROW * cell_width / (2.0 * jnp.pi)
    angle = 2.0 * jnp.pi * row_index / N_ROW
    centre_x = 0.5 + radius * jnp.cos(angle)
    centre_y = 0.5 + radius * jnp.sin(angle)
    centre_z = 0.5 + (target_col - N_COL / 2.0) * 3.0 * cell_width
    centres = jnp.stack([centre_x, centre_y, centre_z])
    leaf_jitter = jax.random.uniform(key_leaf, (3, ROWS // LEAF), jnp.float32, -0.5, 0.5) * cell_width
    slot_offset = jax.random.uniform(key_slot, (3, ROWS), jnp.float32, -0.5, 0.5) * cell_width
    return (centres + leaf_jitter[:, leaf_index] + slot_offset).astype(jnp.float32)


def place_ends(values, rng, low, top_value):
    longest = values.shape.index(max(values.shape))
    spots = []
    for shift in (0, 1):
        where = [jax.random.randint(jax.random.fold_in(rng, axis), (), 0, length) for axis, length in enumerate(values.shape)]
        where[longest] = (where[longest] + shift) % values.shape[longest]
        spots.append(tuple(where))
    return values.at[spots[0]].set(low).at[spots[1]].set(top_value)


def shard_levels(stream_key, shape, cuts, least, high):
    factor_of, own = 1.0, jax.random.fold_in(stream_key, 6)
    for axis_at, blocks in cuts:
        steps = jnp.exp(jax.random.uniform(jax.random.fold_in(own, axis_at), (blocks,), jnp.float32, least / len(cuts), high / len(cuts)))
        factor_of = factor_of * jnp.repeat(steps, shape[axis_at] // blocks).reshape([-1 if axis == axis_at else 1 for axis in range(len(shape))])
    return factor_of


def setup_inputs(seed: int = 0) -> dict:
    streams_of = jax.random.split(jax.random.key(seed), 5)
    positions = draw_positions(jax.random.fold_in(streams_of[4], 71), 0)
    masses = jnp.clip(jnp.exp(math.log(1.999999987845058e-08) - 2.3025851 * jax.random.uniform(streams_of[1], (1, ROWS), jnp.float32) ** shard_levels(streams_of[1], (1, ROWS), ((1, 768),), -0.2, 0.2)), 1.999999943436137e-09, 1.999999987845058e-08)
    counts = place_ends(jax.random.randint(streams_of[2], (1, DEVICES * NL), LEAF // 4, LEAF + 1), jax.random.fold_in(streams_of[2], 1), LEAF // 4, LEAF).astype(jnp.int32)
    sources = draw_sources(jax.random.fold_in(streams_of[4], 71), 0)
    return {"positions": positions, "masses": masses, "counts": counts, "sources": sources}


softening = 2.5e-07

def leaf_forces(full_table, targets, sources, alive):
    count = targets.shape[0]
    width = targets.shape[2]
    target_groups = targets.reshape(count // 8, 8, 4, width)
    source_groups = sources.reshape(count // 8, 8, sources.shape[1])
    alive_groups = alive.reshape(count // 8, 8, width)

    def one_group(items):
        target, index, living = items
        source = full_table[index]
        delta_x = source[:, :, 0, None, :] - target[:, None, 0, :, None]
        delta_y = source[:, :, 1, None, :] - target[:, None, 1, :, None]
        delta_z = source[:, :, 2, None, :] - target[:, None, 2, :, None]
        spread = softening + delta_x * delta_x + delta_y * delta_y + delta_z * delta_z
        weight = source[:, :, 3, None, :] / (spread * jnp.sqrt(spread))
        pull_x = lax.optimization_barrier(jnp.sum(weight * delta_x, axis=(1, 3)))
        pull_y = lax.optimization_barrier(jnp.sum(weight * delta_y, axis=(1, 3)))
        pull_z = lax.optimization_barrier(jnp.sum(weight * delta_z, axis=(1, 3)))
        return jnp.stack([pull_x, pull_y, pull_z], axis=1) * living[:, None, :]
    out = lax.map(one_group, (target_groups, source_groups, alive_groups))
    return out.reshape(count, 3, width)

def reference(positions, masses, counts, sources):
    rows_n, cols_n = (N_ROW, N_COL)
    coords = positions.reshape(3, rows_n, cols_n, cols_n, BLK, LEAF).transpose(1, 3, 2, 4, 0, 5).reshape(rows_n, cols_n, NL, 3, LEAF)
    weights = masses.reshape(1, rows_n, cols_n, cols_n, BLK, LEAF).transpose(1, 3, 2, 4, 0, 5).reshape(rows_n, cols_n, NL, 1, LEAF)
    livecount = counts.reshape(rows_n, cols_n, cols_n, BLK).transpose(0, 2, 1, 3).reshape(rows_n, cols_n, NL)
    alive = (jnp.arange(LEAF, dtype=jnp.int32)[None, None, None, :] < livecount[..., None]).astype(jnp.float32)
    table = jnp.concatenate([coords, weights * alive[:, :, :, None, :]], axis=3)
    full = jnp.concatenate([table, jnp.roll(table, 1, axis=0), jnp.roll(table, -1, axis=0)], axis=2)
    full = full.reshape(rows_n * cols_n, 3 * NL, 4, LEAF)
    lists = sources.reshape(rows_n * cols_n, NL, K)
    alive_all = alive.reshape(rows_n * cols_n, NL, LEAF)

    def device_forces(items):
        whole, index, living = items
        return leaf_forces(whole, whole[:NL], index, living)
    result = lax.map(device_forces, (full, lists, alive_all))
    return result.transpose(2, 0, 1, 3).reshape(3, ROWS)
```

```python
import jax
import jax.numpy as jnp
from jax import lax
from jax.experimental import pallas as pl
from jax.experimental.pallas import tpu as pltpu
from jax.sharding import PartitionSpec as P

softening = 2.5e-07
LEAVES = 128
SLOTS = 128
NEAR = 32
DEAD = -1.0
MIB = 1024 * 1024


def pack_kernel(positions, masses, counts, out):
    lane = lax.broadcasted_iota(jnp.int32, (1, SLOTS), 1)

    def group(first, _):
        for part in range(8):
            leaf = first * 8 + part
            at = pl.multiple_of(leaf * SLOTS, SLOTS)
            out[leaf, 0:3, :] = positions[:, pl.ds(at, SLOTS)]
            out[leaf, 3:4, :] = jnp.where(lane < counts[0, leaf], masses[:, pl.ds(at, SLOTS)], DEAD)
        return 0

    lax.fori_loop(0, LEAVES // 8, group, 0)


def plan_kernel(sources, slot_of, picked):
    low = lax.broadcasted_iota(jnp.int32, (2 * LEAVES, SLOTS), 0) + LEAVES
    named = jnp.zeros((2 * LEAVES, SLOTS), jnp.bool_)
    for k in range(8):
        named = named | (low == sources[k : k + 1, :])
    flags = named.astype(jnp.float32).astype(jnp.bfloat16)
    ones = jnp.ones((8, SLOTS), jnp.bfloat16)
    lanes = (((1,), (1,)), ((), ()))
    uses = lax.dot_general(ones, flags, lanes, preferred_element_type=jnp.float32)
    present = uses > 0.5
    row = lax.broadcasted_iota(jnp.int32, (2 * LEAVES, 2 * LEAVES), 0)
    col = lax.broadcasted_iota(jnp.int32, (2 * LEAVES, 2 * LEAVES), 1)
    before = (row < col).astype(jnp.float32).astype(jnp.bfloat16)
    ahead = present.astype(jnp.float32).astype(jnp.bfloat16)
    rank = lax.dot_general(ahead, before, (((1,), (0,)), ((), ())), preferred_element_type=jnp.float32)
    rank = rank.astype(jnp.int32)
    slot_of[...] = jnp.minimum(rank, 2 * NEAR - 1)
    slot = lax.broadcasted_iota(jnp.int32, (SLOTS, 2 * LEAVES), 0)
    chosen = (slot == jnp.where(present, rank, -1)[0:1, :]).astype(jnp.float32).astype(jnp.bfloat16)
    leaf = lax.broadcasted_iota(jnp.int32, (8, 2 * LEAVES), 1) & (LEAVES - 1)
    leaf = leaf.astype(jnp.float32).astype(jnp.bfloat16)
    picked[...] = lax.dot_general(leaf, chosen, lanes, preferred_element_type=jnp.float32).astype(jnp.int32)


def pair_forces(source_table, target_table, ids, spread, sums, stage, chunks_vmem, chunks_smem, sem, leaves):
    null_chunk = leaves * 8
    ones = jnp.ones((8, SLOTS), jnp.bfloat16)
    live = (source_table[:, 3, :] >= 0.0).astype(jnp.float32).astype(jnp.bfloat16)
    if leaves < SLOTS:
        live = jnp.concatenate([live, jnp.zeros((SLOTS - leaves, SLOTS), jnp.bfloat16)], axis=0)
    count = lax.dot_general(ones, live, (((1,), (1,)), ((), ())), preferred_element_type=jnp.float32)
    size = (count.astype(jnp.int32) + 15) >> 4
    mine = ids >= 0
    leaf = jnp.where(mine, ids, 0)
    size = jnp.where(mine, jnp.take_along_axis(size, leaf, axis=1), 0)
    sub = lax.broadcasted_iota(jnp.int32, (8, SLOTS), 0)
    starts, shifts, total = [], [], jnp.zeros((8, SLOTS), jnp.int32)
    for k in range(8):
        starts.append(total)
        shifts.append(jnp.broadcast_to(leaf[k : k + 1, :], (8, SLOTS)) * 8 - total)
        total = total + jnp.broadcast_to(size[k : k + 1, :], (8, SLOTS))
    for part in range(8):
        at = sub + 8 * part
        chunk = at + shifts[0]
        for k in range(1, 8):
            chunk = jnp.where(at >= starts[k], at + shifts[k], chunk)
        chunks_vmem[8 * part : 8 * part + 8, :] = jnp.where(at < total, chunk, null_chunk)
    chunks_vmem[64:72, :] = total
    to_scalars = pltpu.make_async_copy(chunks_vmem, chunks_smem, sem)
    to_scalars.start()

    unit = 4

    def spread_leaf(first, _):
        rows = []
        for u in range(unit):
            for c in range(4):
                row = source_table[first * unit + u, c : c + 1, :]
                rows.append(jnp.broadcast_to(jnp.maximum(row, 0.0) if c == 3 else row, (8, SLOTS)))
        for block in range(16):
            index = sub + 8 * block
            for u in range(unit):
                for c in range(4):
                    spread[(first * unit + u) * 16 + block, 8 * c : 8 * c + 8, :] = jnp.take_along_axis(
                        rows[u * 4 + c], index, axis=1
                    )
        return 0

    lax.fori_loop(0, leaves // unit, spread_leaf, 0)
    for block in range(2):
        spread[leaves * 16 + block] = jnp.zeros((32, SLOTS), jnp.float32)
    stage[:, 0:32, :] = jnp.zeros((8, 32, SLOTS), jnp.float32)
    stage[:, 32:40, :] = jnp.ones((8, 8, SLOTS), jnp.float32)

    def clear(i, _):
        for part in range(8):
            sums[i * 8 + part] = jnp.zeros((24, SLOTS), jnp.float32)
        return 0

    lax.fori_loop(0, LEAVES // 8, clear, 0)
    to_scalars.wait()

    def staged(u):
        return [stage[u, 8 * c : 8 * c + 8, :] for c in range(4)]

    def add_staged(old, r, pulls):
        weight = (old[3] * r) * (r * r)
        parts = [weight * old[c] for c in range(3)]
        return parts if pulls is None else [a + b for a, b in zip(pulls, parts)]

    def fill_stage(u, block, centre):
        dx, dy, dz = (spread[block, 8 * c : 8 * c + 8, :] - centre[c] for c in range(3))
        stage[u, 0:8, :] = dx
        stage[u, 8:16, :] = dy
        stage[u, 16:24, :] = dz
        stage[u, 24:32, :] = spread[block, 24:32, :]
        stage[u, 32:40, :] = (dx * dx + softening) + (dy * dy + dz * dz)

    def add_to_sums(target, pulls):
        for c in range(3):
            sums[target, 8 * c : 8 * c + 8, :] += pulls[c]

    def chunks_at(target, at):
        return tuple(chunks_smem[at + i, target] * 2 for i in range(4))

    def body(state):
        target, at, old_target, chunks = state
        centre = [jnp.broadcast_to(target_table[target, c : c + 1, :], (8, SLOTS)) for c in range(3)]
        roots = [lax.rsqrt(stage[u, 32:40, :]) for u in range(8)]
        pulls = None
        for u in range(8):
            old = staged(u)
            fill_stage(u, chunks[u // 2] + u % 2, centre)
            pulls = add_staged(old, roots[u], pulls)
        add_to_sums(old_target, pulls)
        done = at + 4 >= chunks_smem[64, target]
        after = jnp.where(done, target + 1, target)
        at = jnp.where(done, 0, at + 4)
        return after, at, target, chunks_at(jnp.minimum(after, LEAVES - 1), at)

    zero = jnp.int32(0)
    state = lax.while_loop(lambda s: s[0] < LEAVES, body, (zero, zero, zero, chunks_at(zero, zero)))
    pulls = None
    for u in range(8):
        pulls = add_staged(staged(u), lax.rsqrt(stage[u, 32:40, :]), pulls)
    add_to_sums(state[2], pulls)


def own_kernel(table, sources, out, spread, sums, stage, chunks_vmem, chunks_smem, sem):
    ids = sources[...]
    ids = jnp.where(ids < LEAVES, ids, -1)
    pair_forces(table, table, ids, spread, sums, stage, chunks_vmem, chunks_smem, sem, LEAVES)

    def finish(i, _):
        for part in range(8):
            t = i * 8 + part
            for c in range(3):
                out[t, c : c + 1, :] = jnp.sum(sums[t, 8 * c : 8 * c + 8, :], axis=0, keepdims=True)
        return 0

    lax.fori_loop(0, LEAVES // 8, finish, 0)


def near_kernel(before, after, table, own_pull, sources, slot_of, picked, out, leaves, spread, sums, stage, chunks_vmem, chunks_smem, sem):
    def gather(i, _):
        for part in range(8):
            s = i * 8 + part
            leaves[s] = before[picked[0, s]]
            leaves[NEAR + s] = after[picked[0, NEAR + s]]
        return 0

    lax.fori_loop(0, NEAR // 8, gather, 0)
    ids = sources[...]
    within = ids & (LEAVES - 1)
    below = jnp.take_along_axis(slot_of[:, :LEAVES], within, axis=1)
    above = jnp.take_along_axis(slot_of[:, LEAVES:], within, axis=1)
    ids = jnp.where(ids < LEAVES, -1, jnp.where(ids < 2 * LEAVES, below, above))
    pair_forces(leaves, table, ids, spread, sums, stage, chunks_vmem, chunks_smem, sem, 2 * NEAR)

    def finish(i, _):
        for part in range(8):
            t = i * 8 + part
            at = pl.multiple_of(t * SLOTS, SLOTS)
            living = table[t, 3:4, :] >= 0.0
            for c in range(3):
                pull = jnp.sum(sums[t, 8 * c : 8 * c + 8, :], axis=0, keepdims=True) + own_pull[t, c : c + 1, :]
                out[c : c + 1, pl.ds(at, SLOTS)] = jnp.where(living, pull, 0.0)
        return 0

    lax.fori_loop(0, LEAVES // 8, finish, 0)


def f32(*shape):
    return jax.ShapeDtypeStruct(shape, jnp.float32)


def i32(*shape):
    return jax.ShapeDtypeStruct(shape, jnp.int32)


vmem = pl.BlockSpec(memory_space=pltpu.VMEM)
smem = pl.BlockSpec(memory_space=pltpu.SMEM)


def pair_scratch(leaves):
    return [
        pltpu.VMEM((leaves * 16 + 2, 32, SLOTS), jnp.float32),
        pltpu.VMEM((LEAVES, 24, SLOTS), jnp.float32),
        pltpu.VMEM((8, 40, SLOTS), jnp.float32),
        pltpu.VMEM((72, SLOTS), jnp.int32),
        pltpu.SMEM((72, SLOTS), jnp.int32),
        pltpu.SemaphoreType.DMA,
    ]


def cost(us):
    return pl.CostEstimate(flops=int(us * 8_000_000), bytes_accessed=0, transcendentals=0)


def pack(positions, masses, counts):
    return pl.pallas_call(
        pack_kernel,
        out_shape=f32(LEAVES, 4, SLOTS),
        in_specs=[vmem, vmem, smem],
        out_specs=vmem,
        name="pack",
    )(positions, masses, counts)


def plan(sources):
    return pl.pallas_call(
        plan_kernel,
        out_shape=(i32(8, 2 * LEAVES), i32(8, SLOTS)),
        in_specs=[vmem],
        out_specs=(vmem, vmem),
        cost_estimate=cost(1),
        name="plan",
    )(sources)


def own_forces(table, sources):
    return pl.pallas_call(
        own_kernel,
        out_shape=f32(LEAVES, 4, SLOTS),
        in_specs=[vmem, vmem],
        out_specs=vmem,
        scratch_shapes=pair_scratch(LEAVES),
        compiler_params=pltpu.CompilerParams(vmem_limit_bytes=42 * MIB),
        cost_estimate=cost(20),
        name="own_forces",
    )(table, sources)


def near_forces(before, after, table, own_pull, sources, slot_of, picked):
    return pl.pallas_call(
        near_kernel,
        out_shape=f32(3, LEAVES * SLOTS),
        in_specs=[vmem, vmem, vmem, vmem, vmem, vmem, smem],
        out_specs=vmem,
        scratch_shapes=[pltpu.VMEM((2 * NEAR, 4, SLOTS), jnp.float32)] + pair_scratch(2 * NEAR),
        compiler_params=pltpu.CompilerParams(vmem_limit_bytes=30 * MIB),
        cost_estimate=cost(12),
        name="near_forces",
    )(before, after, table, own_pull, sources, slot_of, picked)


def on_device(positions, masses, counts, sources):
    sources = sources.T
    sent = pack(positions, masses, counts)
    slot_of, picked = plan(sources)
    table = lax.all_to_all(sent, "col", split_axis=0, concat_axis=0, tiled=True)
    size = lax.axis_size("row")
    up = [(i, (i + 1) % size) for i in range(size)]
    down = [(j, i) for i, j in up]
    before = lax.ppermute(table, "row", up)
    after = lax.ppermute(table, "row", down)
    own_pull = own_forces(table, sources)
    return near_forces(before, after, table, own_pull, sources, slot_of, picked)


def solution(mesh):
    return jax.shard_map(
        on_device,
        mesh=mesh,
        in_specs=(
            P(None, ("row", "col")),
            P(None, ("row", "col")),
            P(None, ("row", "col")),
            P(("row", "col"), None),
        ),
        out_specs=P(None, ("row", "col")),
        check_vma=False,
    )
```

```python
import jax
import jax.numpy as jnp
from jax import lax
from jax.experimental import pallas as pl
from jax.experimental.pallas import tpu as pltpu
from jax.sharding import PartitionSpec as P

softening = 2.5e-07
unit = 16
blocks = 8
LEAVES = 128
SLOTS = 128
NEAR = 32
DEAD = -1.0
MIB = 1024 * 1024


def pack_kernel(positions, masses, counts, out):
    lane = lax.broadcasted_iota(jnp.int32, (1, SLOTS), 1)

    def group(first, _):
        for part in range(8):
            leaf = first * 8 + part
            at = pl.multiple_of(leaf * SLOTS, SLOTS)
            out[leaf, 0:3, :] = positions[:, pl.ds(at, SLOTS)]
            out[leaf, 3:4, :] = jnp.where(lane < counts[0, leaf], masses[:, pl.ds(at, SLOTS)], DEAD)
        return 0

    lax.fori_loop(0, LEAVES // 8, group, 0)


def number_neighbours(sources, slot_of, picked):
    low = lax.broadcasted_iota(jnp.int32, (2 * LEAVES, SLOTS), 0) + LEAVES
    named = jnp.zeros((2 * LEAVES, SLOTS), jnp.bool_)
    for k in range(8):
        named = named | (low == sources[k : k + 1, :])
    flags = named.astype(jnp.float32).astype(jnp.bfloat16)
    ones = jnp.ones((8, SLOTS), jnp.bfloat16)
    lanes = (((1,), (1,)), ((), ()))
    uses = lax.dot_general(ones, flags, lanes, preferred_element_type=jnp.float32)
    present = uses > 0.5
    row = lax.broadcasted_iota(jnp.int32, (2 * LEAVES, 2 * LEAVES), 0)
    col = lax.broadcasted_iota(jnp.int32, (2 * LEAVES, 2 * LEAVES), 1)
    before = (row < col).astype(jnp.float32).astype(jnp.bfloat16)
    ahead = present.astype(jnp.float32).astype(jnp.bfloat16)
    rank = lax.dot_general(ahead, before, (((1,), (0,)), ((), ())), preferred_element_type=jnp.float32)
    rank = rank.astype(jnp.int32)
    slot_of[...] = jnp.minimum(rank, 2 * NEAR - 1)
    slot = lax.broadcasted_iota(jnp.int32, (SLOTS, 2 * LEAVES), 0)
    chosen = (slot == jnp.where(present, rank, -1)[0:1, :]).astype(jnp.float32).astype(jnp.bfloat16)
    leaf = lax.broadcasted_iota(jnp.int32, (8, 2 * LEAVES), 1) & (LEAVES - 1)
    leaf = leaf.astype(jnp.float32).astype(jnp.bfloat16)
    picked[...] = lax.dot_general(leaf, chosen, lanes, preferred_element_type=jnp.float32).astype(jnp.int32)


def pair_forces(source_table, target_table, ids, spread, sums, chunks_vmem, chunks_smem, sem, leaves):
    null_chunk = leaves * 8
    ones = jnp.ones((8, SLOTS), jnp.bfloat16)
    live = (source_table[:, 3, :] >= 0.0).astype(jnp.float32).astype(jnp.bfloat16)
    if leaves < SLOTS:
        live = jnp.concatenate([live, jnp.zeros((SLOTS - leaves, SLOTS), jnp.bfloat16)], axis=0)
    count = lax.dot_general(ones, live, (((1,), (1,)), ((), ())), preferred_element_type=jnp.float32)
    size = (count.astype(jnp.int32) + 15) >> 4
    mine = ids >= 0
    leaf = jnp.where(mine, ids, 0)
    size = jnp.where(mine, jnp.take_along_axis(size, leaf, axis=1), 0)
    sub = lax.broadcasted_iota(jnp.int32, (8, SLOTS), 0)
    starts, shifts, total = [], [], jnp.zeros((8, SLOTS), jnp.int32)
    for k in range(8):
        starts.append(total)
        shifts.append(jnp.broadcast_to(leaf[k : k + 1, :], (8, SLOTS)) * 8 - total)
        total = total + jnp.broadcast_to(size[k : k + 1, :], (8, SLOTS))
    for part in range(8):
        at = sub + 8 * part
        chunk = at + shifts[0]
        for k in range(1, 8):
            chunk = jnp.where(at >= starts[k], at + shifts[k], chunk)
        chunks_vmem[8 * part : 8 * part + 8, :] = jnp.where(at < total, chunk, null_chunk)
    chunks_vmem[64:72, :] = total
    chunks_vmem[72:80, :] = jnp.full((8, SLOTS), null_chunk, jnp.int32)
    to_scalars = pltpu.make_async_copy(chunks_vmem, chunks_smem, sem)
    to_scalars.start()

    limb = lax.broadcasted_iota(jnp.int32, (16, 4 * SLOTS), 0)
    column = lax.broadcasted_iota(jnp.int32, (16, 4 * SLOTS), 1)
    gather = ((limb < 12) & ((limb & 3) == column // SLOTS)).astype(jnp.float32).astype(jnp.bfloat16)

    def limbs_of(tile):
        high = tile.astype(jnp.bfloat16).astype(jnp.float32)
        rest = tile - high
        middle = rest.astype(jnp.bfloat16).astype(jnp.float32)
        low = rest - middle
        return jnp.concatenate([high, middle, low, jnp.zeros((4, SLOTS), jnp.float32)], axis=0)

    value = lax.broadcasted_iota(jnp.int32, (4, SLOTS), 0)

    def spread_leaf(first, _):
        lhs = []
        for u in range(unit):
            tile = source_table[first * unit + u]
            tile = jnp.where(value == 3, jnp.maximum(tile, 0.0), tile)
            lhs.append(jnp.transpose(limbs_of(tile)).astype(jnp.bfloat16))
        at = pl.multiple_of(first * (unit * SLOTS), unit * SLOTS)
        spread[pl.ds(at, unit * SLOTS), :] = jnp.dot(
            jnp.concatenate(lhs, axis=0), gather, preferred_element_type=jnp.float32
        )
        return 0

    lax.fori_loop(0, leaves // unit, spread_leaf, 0)
    spread[leaves * SLOTS : leaves * SLOTS + 16, :] = jnp.zeros((16, 4 * SLOTS), jnp.float32)

    def clear(i, _):
        for part in range(8):
            sums[i * 8 + part] = jnp.zeros((24, SLOTS), jnp.float32)
        return 0

    lax.fori_loop(0, LEAVES // 8, clear, 0)
    to_scalars.wait()

    def pull_on(target, chunks):
        centre = [jnp.broadcast_to(target_table[target, c : c + 1, :], (8, SLOTS)) for c in range(3)]
        pulls = None
        for u in range(8):
            block = chunks[u // 2] + u % 2
            rows = pl.ds(pl.multiple_of(block * 8, 8), 8)
            delta = [spread[rows, SLOTS * c : SLOTS * c + SLOTS] - centre[c] for c in range(3)]
            squares = [d * d for d in delta]
            r = lax.rsqrt((squares[0] + softening) + (squares[1] + squares[2]))
            weight = (spread[rows, 3 * SLOTS : 4 * SLOTS] * r) * (r * r)
            parts = [weight * d for d in delta]
            pulls = parts if pulls is None else [a + b for a, b in zip(pulls, parts)]
        for c in range(3):
            sums[target, 8 * c : 8 * c + 8, :] += pulls[c]

    def chunks_at(target, at):
        return tuple(chunks_smem[at + i, target] * 2 for i in range(4))

    def body(state):
        target, at, chunks = state
        for _ in range(blocks):
            pull_on(target, chunks)
            at = at + 4
            done = at >= chunks_smem[64, target]
            over = done & (target == LEAVES - 1)
            target = jnp.where(done & ~over, target + 1, target)
            at = jnp.where(over, 72, jnp.where(done, 0, at))
            chunks = chunks_at(target, at)
        return target, at, chunks

    zero = jnp.int32(0)
    lax.while_loop(lambda s: s[1] < 72, body, (zero, zero, chunks_at(zero, zero)))


def own_kernel(table, sources, out, slot_of, picked, spread, sums, chunks_vmem, chunks_smem, sem):
    ids = sources[...]
    ids = jnp.where(ids < LEAVES, ids, -1)
    number_neighbours(sources, slot_of, picked)
    pair_forces(table, table, ids, spread, sums, chunks_vmem, chunks_smem, sem, LEAVES)

    def finish(i, _):
        for part in range(8):
            t = i * 8 + part
            for c in range(3):
                out[t, c : c + 1, :] = jnp.sum(sums[t, 8 * c : 8 * c + 8, :], axis=0, keepdims=True)
        return 0

    lax.fori_loop(0, LEAVES // 8, finish, 0)


def near_kernel(before, after, table, own_pull, sources, slot_of, picked, out, leaves, spread, sums, chunks_vmem, chunks_smem, sem):
    def gather(i, _):
        for part in range(8):
            s = i * 8 + part
            leaves[s] = before[picked[0, s]]
            leaves[NEAR + s] = after[picked[0, NEAR + s]]
        return 0

    lax.fori_loop(0, NEAR // 8, gather, 0)
    ids = sources[...]
    within = ids & (LEAVES - 1)
    below = jnp.take_along_axis(slot_of[:, :LEAVES], within, axis=1)
    above = jnp.take_along_axis(slot_of[:, LEAVES:], within, axis=1)
    ids = jnp.where(ids < LEAVES, -1, jnp.where(ids < 2 * LEAVES, below, above))
    pair_forces(leaves, table, ids, spread, sums, chunks_vmem, chunks_smem, sem, 2 * NEAR)

    def finish(i, _):
        for part in range(8):
            t = i * 8 + part
            at = pl.multiple_of(t * SLOTS, SLOTS)
            living = table[t, 3:4, :] >= 0.0
            for c in range(3):
                pull = jnp.sum(sums[t, 8 * c : 8 * c + 8, :], axis=0, keepdims=True) + own_pull[t, c : c + 1, :]
                out[c : c + 1, pl.ds(at, SLOTS)] = jnp.where(living, pull, 0.0)
        return 0

    lax.fori_loop(0, LEAVES // 8, finish, 0)


def f32(*shape):
    return jax.ShapeDtypeStruct(shape, jnp.float32)


def i32(*shape):
    return jax.ShapeDtypeStruct(shape, jnp.int32)


vmem = pl.BlockSpec(memory_space=pltpu.VMEM)
smem = pl.BlockSpec(memory_space=pltpu.SMEM)


def pair_scratch(leaves):
    return [
        pltpu.VMEM((leaves * SLOTS + 16, 4 * SLOTS), jnp.float32),
        pltpu.VMEM((LEAVES, 24, SLOTS), jnp.float32),
        pltpu.VMEM((80, SLOTS), jnp.int32),
        pltpu.SMEM((80, SLOTS), jnp.int32),
        pltpu.SemaphoreType.DMA,
    ]


def cost(us):
    return pl.CostEstimate(flops=int(us * 8_000_000), bytes_accessed=0, transcendentals=0)


def pack(positions, masses, counts):
    return pl.pallas_call(
        pack_kernel,
        out_shape=f32(LEAVES, 4, SLOTS),
        in_specs=[vmem, vmem, smem],
        out_specs=vmem,
        name="pack",
    )(positions, masses, counts)


def own_forces(table, sources):
    return pl.pallas_call(
        own_kernel,
        out_shape=(f32(LEAVES, 4, SLOTS), i32(8, 2 * LEAVES), i32(8, SLOTS)),
        in_specs=[vmem, vmem],
        out_specs=(vmem, vmem, vmem),
        scratch_shapes=pair_scratch(LEAVES),
        compiler_params=pltpu.CompilerParams(vmem_limit_bytes=42 * MIB),
        cost_estimate=cost(20),
        name="own_forces",
    )(table, sources)


def near_forces(before, after, table, own_pull, sources, slot_of, picked):
    return pl.pallas_call(
        near_kernel,
        out_shape=f32(3, LEAVES * SLOTS),
        in_specs=[vmem, vmem, vmem, vmem, vmem, vmem, smem],
        out_specs=vmem,
        scratch_shapes=[pltpu.VMEM((2 * NEAR, 4, SLOTS), jnp.float32)] + pair_scratch(2 * NEAR),
        compiler_params=pltpu.CompilerParams(vmem_limit_bytes=30 * MIB),
        cost_estimate=cost(12),
        name="near_forces",
    )(before, after, table, own_pull, sources, slot_of, picked)


def on_device(positions, masses, counts, sources):
    sources = sources.T
    sent = pack(positions, masses, counts)
    table = lax.all_to_all(sent, "col", split_axis=0, concat_axis=0, tiled=True)
    size = lax.axis_size("row")
    up = [(i, (i + 1) % size) for i in range(size)]
    down = [(j, i) for i, j in up]
    before = lax.ppermute(table, "row", up)
    after = lax.ppermute(table, "row", down)
    own_pull, slot_of, picked = own_forces(table, sources)
    return near_forces(before, after, table, own_pull, sources, slot_of, picked)


def solution(mesh):
    return jax.shard_map(
        on_device,
        mesh=mesh,
        in_specs=(
            P(None, ("row", "col")),
            P(None, ("row", "col")),
            P(None, ("row", "col")),
            P(("row", "col"), None),
        ),
        out_specs=P(None, ("row", "col")),
        check_vma=False,
    )
```

```python
import jax
import jax.numpy as jnp
from jax import lax
from jax.experimental import pallas as pl
from jax.experimental.pallas import tpu as pltpu
from jax.sharding import PartitionSpec as P

softening = 2.5e-07
unit = 32
SHIFT = 3
ROWS = 1 << SHIFT
width = 8
blocks = 12
LEAVES = 128
SLOTS = 128
NEAR = 32
DEAD = -1.0
MIB = 1024 * 1024


def pack_kernel(positions, masses, counts, out):
    lane = lax.broadcasted_iota(jnp.int32, (1, SLOTS), 1)

    def group(first, _):
        for part in range(8):
            leaf = first * 8 + part
            at = pl.multiple_of(leaf * SLOTS, SLOTS)
            out[leaf, 0:3, :] = positions[:, pl.ds(at, SLOTS)]
            out[leaf, 3:4, :] = jnp.where(lane < counts[0, leaf], masses[:, pl.ds(at, SLOTS)], DEAD)
        return 0

    lax.fori_loop(0, LEAVES // 8, group, 0)


def number_neighbours(sources, slot_of, picked):
    low = lax.broadcasted_iota(jnp.int32, (2 * LEAVES, SLOTS), 0) + LEAVES
    named = jnp.zeros((2 * LEAVES, SLOTS), jnp.bool_)
    for k in range(8):
        named = named | (low == sources[k : k + 1, :])
    flags = named.astype(jnp.float32).astype(jnp.bfloat16)
    ones = jnp.ones((8, SLOTS), jnp.bfloat16)
    lanes = (((1,), (1,)), ((), ()))
    uses = lax.dot_general(ones, flags, lanes, preferred_element_type=jnp.float32)
    present = uses > 0.5
    row = lax.broadcasted_iota(jnp.int32, (2 * LEAVES, 2 * LEAVES), 0)
    col = lax.broadcasted_iota(jnp.int32, (2 * LEAVES, 2 * LEAVES), 1)
    before = (row < col).astype(jnp.float32).astype(jnp.bfloat16)
    ahead = present.astype(jnp.float32).astype(jnp.bfloat16)
    rank = lax.dot_general(ahead, before, (((1,), (0,)), ((), ())), preferred_element_type=jnp.float32)
    rank = rank.astype(jnp.int32)
    slot_of[...] = jnp.minimum(rank, 2 * NEAR - 1)
    slot = lax.broadcasted_iota(jnp.int32, (SLOTS, 2 * LEAVES), 0)
    chosen = (slot == jnp.where(present, rank, -1)[0:1, :]).astype(jnp.float32).astype(jnp.bfloat16)
    leaf = lax.broadcasted_iota(jnp.int32, (8, 2 * LEAVES), 1) & (LEAVES - 1)
    leaf = leaf.astype(jnp.float32).astype(jnp.bfloat16)
    picked[...] = lax.dot_general(leaf, chosen, lanes, preferred_element_type=jnp.float32).astype(jnp.int32)


def pair_forces(source_table, target_table, ids, spread, sums, chunks_vmem, chunks_smem, sem, leaves):
    per_leaf = SLOTS // ROWS
    most = 8 * per_leaf
    null_chunk = leaves * per_leaf
    ones = jnp.ones((8, SLOTS), jnp.bfloat16)
    live = (source_table[:, 3, :] >= 0.0).astype(jnp.float32).astype(jnp.bfloat16)
    if leaves < SLOTS:
        live = jnp.concatenate([live, jnp.zeros((SLOTS - leaves, SLOTS), jnp.bfloat16)], axis=0)
    count = lax.dot_general(ones, live, (((1,), (1,)), ((), ())), preferred_element_type=jnp.float32)
    size = (count.astype(jnp.int32) + (ROWS - 1)) >> SHIFT
    mine = ids >= 0
    leaf = jnp.where(mine, ids, 0)
    size = jnp.where(mine, jnp.take_along_axis(size, leaf, axis=1), 0)
    sub = lax.broadcasted_iota(jnp.int32, (8, SLOTS), 0)
    starts, shifts, total = [], [], jnp.zeros((8, SLOTS), jnp.int32)
    for k in range(8):
        starts.append(total)
        shifts.append(jnp.broadcast_to(leaf[k : k + 1, :], (8, SLOTS)) * per_leaf - total)
        total = total + jnp.broadcast_to(size[k : k + 1, :], (8, SLOTS))
    for part in range(per_leaf):
        at = sub + 8 * part
        chunk = at + shifts[0]
        for k in range(1, 8):
            chunk = jnp.where(at >= starts[k], at + shifts[k], chunk)
        chunks_vmem[pl.ds(1024 * part, 1024)] = jnp.where(at < total, chunk, null_chunk).reshape(1024)
    target_of = lax.broadcasted_iota(jnp.int32, (8, SLOTS), 1)
    chunks_vmem[pl.ds(SLOTS * most, 1024)] = (total * SLOTS + target_of).reshape(1024)
    chunks_vmem[pl.ds(SLOTS * most + 1024, 1024)] = jnp.full((1024,), null_chunk, jnp.int32)
    to_scalars = pltpu.make_async_copy(chunks_vmem, chunks_smem, sem)
    to_scalars.start()

    limb = lax.broadcasted_iota(jnp.int32, (16, 4 * SLOTS), 0)
    column = lax.broadcasted_iota(jnp.int32, (16, 4 * SLOTS), 1)
    gather = ((limb < 12) & ((limb & 3) == column // SLOTS)).astype(jnp.float32).astype(jnp.bfloat16)

    def limbs_of(tile):
        high = tile.astype(jnp.bfloat16).astype(jnp.float32)
        rest = tile - high
        middle = rest.astype(jnp.bfloat16).astype(jnp.float32)
        low = rest - middle
        return jnp.concatenate([high, middle, low, jnp.zeros((4, SLOTS), jnp.float32)], axis=0)

    value = lax.broadcasted_iota(jnp.int32, (4, SLOTS), 0)

    def spread_leaf(first, _):
        lhs = []
        for u in range(unit):
            tile = source_table[first * unit + u]
            tile = jnp.where(value == 3, jnp.maximum(tile, 0.0), tile)
            lhs.append(jnp.transpose(limbs_of(tile)).astype(jnp.bfloat16))
        copied = jnp.dot(jnp.concatenate(lhs, axis=0), gather, preferred_element_type=jnp.float32)
        pieces = unit * SLOTS // ROWS
        spread[pl.ds(first * pieces, pieces)] = copied.reshape(pieces, ROWS, 4 * SLOTS)
        return 0

    lax.fori_loop(0, leaves // unit, spread_leaf, 0)
    spread[null_chunk] = jnp.zeros((ROWS, 4 * SLOTS), jnp.float32)

    def clear(i, _):
        for part in range(8):
            sums[i * 8 + part] = jnp.zeros((24, SLOTS), jnp.float32)
        return 0

    lax.fori_loop(0, LEAVES // 8, clear, 0)
    to_scalars.wait()

    def pull_on(target, chunks):
        centre = [jnp.broadcast_to(target_table[target, c : c + 1, :], (8, SLOTS)) for c in range(3)]
        pulls = None
        for chunk in chunks:
            for row in range(0, ROWS, 8):
                piece = [spread[chunk, row : row + 8, SLOTS * c : SLOTS * c + SLOTS] for c in range(4)]
                delta = [piece[c] - centre[c] for c in range(3)]
                squares = [d * d for d in delta]
                r = lax.rsqrt((squares[0] + softening) + (squares[1] + squares[2]))
                weight = (piece[3] * r) * (r * r)
                parts = [weight * d for d in delta]
                pulls = parts if pulls is None else [a + b for a, b in zip(pulls, parts)]
        for c in range(3):
            sums[target, 8 * c : 8 * c + 8, :] += pulls[c]

    def chunks_at(at):
        return tuple(chunks_smem[at + i * SLOTS] for i in range(width))

    finished = SLOTS * most + 1024 + LEAVES - 1

    def body(state):
        target, at, chunks = state
        for _ in range(blocks):
            pull_on(target, chunks)
            at = at + width * SLOTS
            done = at >= chunks_smem[SLOTS * most + target]
            over = done & (target == LEAVES - 1)
            target = jnp.where(done & ~over, target + 1, target)
            at = jnp.where(over, finished, jnp.where(done, target, at))
            chunks = chunks_at(at)
        return target, at, chunks

    zero = jnp.int32(0)
    lax.while_loop(lambda s: s[1] < finished, body, (zero, zero, chunks_at(zero)))


def own_kernel(table, sources, out, slot_of, picked, spread, sums, chunks_vmem, chunks_smem, sem):
    ids = sources[...]
    ids = jnp.where(ids < LEAVES, ids, -1)
    number_neighbours(sources, slot_of, picked)
    pair_forces(table, table, ids, spread, sums, chunks_vmem, chunks_smem, sem, LEAVES)

    def finish(i, _):
        for part in range(8):
            t = i * 8 + part
            for c in range(3):
                out[t, c : c + 1, :] = jnp.sum(sums[t, 8 * c : 8 * c + 8, :], axis=0, keepdims=True)
        return 0

    lax.fori_loop(0, LEAVES // 8, finish, 0)


def near_kernel(before, after, table, own_pull, sources, slot_of, picked, out, leaves, spread, sums, chunks_vmem, chunks_smem, sem):
    def gather(i, _):
        for part in range(8):
            s = i * 8 + part
            leaves[s] = before[picked[0, s]]
            leaves[NEAR + s] = after[picked[0, NEAR + s]]
        return 0

    lax.fori_loop(0, NEAR // 8, gather, 0)
    ids = sources[...]
    within = ids & (LEAVES - 1)
    below = jnp.take_along_axis(slot_of[:, :LEAVES], within, axis=1)
    above = jnp.take_along_axis(slot_of[:, LEAVES:], within, axis=1)
    ids = jnp.where(ids < LEAVES, -1, jnp.where(ids < 2 * LEAVES, below, above))
    pair_forces(leaves, table, ids, spread, sums, chunks_vmem, chunks_smem, sem, 2 * NEAR)

    def finish(i, _):
        for part in range(8):
            t = i * 8 + part
            at = pl.multiple_of(t * SLOTS, SLOTS)
            living = table[t, 3:4, :] >= 0.0
            for c in range(3):
                pull = jnp.sum(sums[t, 8 * c : 8 * c + 8, :], axis=0, keepdims=True) + own_pull[t, c : c + 1, :]
                out[c : c + 1, pl.ds(at, SLOTS)] = jnp.where(living, pull, 0.0)
        return 0

    lax.fori_loop(0, LEAVES // 8, finish, 0)


def f32(*shape):
    return jax.ShapeDtypeStruct(shape, jnp.float32)


def i32(*shape):
    return jax.ShapeDtypeStruct(shape, jnp.int32)


vmem = pl.BlockSpec(memory_space=pltpu.VMEM)
smem = pl.BlockSpec(memory_space=pltpu.SMEM)


def pair_scratch(leaves):
    return [
        pltpu.VMEM((leaves * (SLOTS // ROWS) + 1, ROWS, 4 * SLOTS), jnp.float32),
        pltpu.VMEM((LEAVES, 24, SLOTS), jnp.float32),
        pltpu.VMEM((8 * SLOTS * SLOTS // ROWS + 2048,), jnp.int32),
        pltpu.SMEM((8 * SLOTS * SLOTS // ROWS + 2048,), jnp.int32),
        pltpu.SemaphoreType.DMA,
    ]


def cost(us):
    return pl.CostEstimate(flops=int(us * 8_000_000), bytes_accessed=0, transcendentals=0)


def pack(positions, masses, counts):
    return pl.pallas_call(
        pack_kernel,
        out_shape=pltpu.VMEM((LEAVES, 4, SLOTS), jnp.float32),
        in_specs=[vmem, vmem, smem],
        out_specs=vmem,
        name="pack",
    )(positions, masses, counts)


def own_forces(table, sources):
    return pl.pallas_call(
        own_kernel,
        out_shape=(f32(LEAVES, 4, SLOTS), i32(8, 2 * LEAVES), i32(8, SLOTS)),
        in_specs=[vmem, vmem],
        out_specs=(vmem, vmem, vmem),
        scratch_shapes=pair_scratch(LEAVES),
        compiler_params=pltpu.CompilerParams(vmem_limit_bytes=42 * MIB),
        cost_estimate=cost(20),
        name="own_forces",
    )(table, sources)


def near_forces(before, after, table, own_pull, sources, slot_of, picked):
    return pl.pallas_call(
        near_kernel,
        out_shape=f32(3, LEAVES * SLOTS),
        in_specs=[vmem, vmem, vmem, vmem, vmem, vmem, smem],
        out_specs=vmem,
        scratch_shapes=[pltpu.VMEM((2 * NEAR, 4, SLOTS), jnp.float32)] + pair_scratch(2 * NEAR),
        compiler_params=pltpu.CompilerParams(vmem_limit_bytes=30 * MIB),
        cost_estimate=cost(12),
        name="near_forces",
    )(before, after, table, own_pull, sources, slot_of, picked)


def on_device(positions, masses, counts, sources):
    sources = sources.T
    sent = pack(positions, masses, counts)
    table = lax.all_to_all(sent, "col", split_axis=0, concat_axis=0, tiled=True)
    size = lax.axis_size("row")
    up = [(i, (i + 1) % size) for i in range(size)]
    down = [(j, i) for i, j in up]
    before = lax.ppermute(table, "row", up)
    after = lax.ppermute(table, "row", down)
    own_pull, slot_of, picked = own_forces(table, sources)
    return near_forces(before, after, table, own_pull, sources, slot_of, picked)


def solution(mesh):
    return jax.shard_map(
        on_device,
        mesh=mesh,
        in_specs=(
            P(None, ("row", "col")),
            P(None, ("row", "col")),
            P(None, ("row", "col")),
            P(("row", "col"), None),
        ),
        out_specs=P(None, ("row", "col")),
        check_vma=False,
    )
```

```python
import jax
import jax.numpy as jnp
from jax import lax
from jax.experimental import pallas as pl
from jax.experimental.pallas import tpu as pltpu
from jax.sharding import PartitionSpec as P

softening = 2.5e-07
SHIFT = 3
ROWS = 1 << SHIFT
width = 8
blocks = 20
LEAVES = 128
SLOTS = 128
NEAR = 32
DEAD = -1.0
MIB = 1024 * 1024


def pack_kernel(positions, masses, counts, out):
    lane = lax.broadcasted_iota(jnp.int32, (1, SLOTS), 1)

    def group(first, _):
        for part in range(8):
            leaf = first * 8 + part
            at = pl.multiple_of(leaf * SLOTS, SLOTS)
            out[leaf, 0:3, :] = positions[:, pl.ds(at, SLOTS)]
            out[leaf, 3:4, :] = jnp.where(lane < counts[0, leaf], masses[:, pl.ds(at, SLOTS)], DEAD)
        return 0

    lax.fori_loop(0, LEAVES // 8, group, 0)


def number_neighbours(sources, slot_of, picked):
    low = lax.broadcasted_iota(jnp.int32, (2 * LEAVES, SLOTS), 0) + LEAVES
    named = jnp.zeros((2 * LEAVES, SLOTS), jnp.bool_)
    for k in range(8):
        named = named | (low == sources[k : k + 1, :])
    flags = named.astype(jnp.float32).astype(jnp.bfloat16)
    ones = jnp.ones((8, SLOTS), jnp.bfloat16)
    lanes = (((1,), (1,)), ((), ()))
    uses = lax.dot_general(ones, flags, lanes, preferred_element_type=jnp.float32)
    present = uses > 0.5
    row = lax.broadcasted_iota(jnp.int32, (2 * LEAVES, 2 * LEAVES), 0)
    col = lax.broadcasted_iota(jnp.int32, (2 * LEAVES, 2 * LEAVES), 1)
    before = (row < col).astype(jnp.float32).astype(jnp.bfloat16)
    ahead = present.astype(jnp.float32).astype(jnp.bfloat16)
    rank = lax.dot_general(ahead, before, (((1,), (0,)), ((), ())), preferred_element_type=jnp.float32)
    rank = rank.astype(jnp.int32)
    slot_of[...] = jnp.minimum(rank, 2 * NEAR - 1)
    slot = lax.broadcasted_iota(jnp.int32, (SLOTS, 2 * LEAVES), 0)
    chosen = (slot == jnp.where(present, rank, -1)[0:1, :]).astype(jnp.float32).astype(jnp.bfloat16)
    leaf = lax.broadcasted_iota(jnp.int32, (8, 2 * LEAVES), 1) & (LEAVES - 1)
    leaf = leaf.astype(jnp.float32).astype(jnp.bfloat16)
    picked[...] = lax.dot_general(leaf, chosen, lanes, preferred_element_type=jnp.float32).astype(jnp.int32)


def clear_sums(sums):
    def clear(i, _):
        for part in range(8):
            sums[i * 8 + part] = jnp.zeros((24, SLOTS), jnp.float32)
        return 0

    lax.fori_loop(0, LEAVES // 8, clear, 0)


def pair_forces(source_table, target_table, ids, spread, sums, chunks_vmem, chunks_smem, sem, leaves):
    per_leaf = SLOTS // ROWS
    most = 8 * per_leaf
    null_chunk = leaves * per_leaf
    ones = jnp.ones((8, SLOTS), jnp.bfloat16)
    live = (source_table[:, 3, :] >= 0.0).astype(jnp.float32).astype(jnp.bfloat16)
    if leaves < SLOTS:
        live = jnp.concatenate([live, jnp.zeros((SLOTS - leaves, SLOTS), jnp.bfloat16)], axis=0)
    count = lax.dot_general(ones, live, (((1,), (1,)), ((), ())), preferred_element_type=jnp.float32)
    size = (count.astype(jnp.int32) + (ROWS - 1)) >> SHIFT
    mine = ids >= 0
    leaf = jnp.where(mine, ids, 0)
    size = jnp.where(mine, jnp.take_along_axis(size, leaf, axis=1), 0)
    sub = lax.broadcasted_iota(jnp.int32, (8, SLOTS), 0)
    starts, shifts, total = [], [], jnp.zeros((8, SLOTS), jnp.int32)
    for k in range(8):
        starts.append(total)
        shifts.append(jnp.broadcast_to(leaf[k : k + 1, :], (8, SLOTS)) * per_leaf - total)
        total = total + jnp.broadcast_to(size[k : k + 1, :], (8, SLOTS))
    groups = most // width
    rows = groups + 8
    target_of = lax.broadcasted_iota(jnp.int32, (8, SLOTS), 1)
    finished = groups * SLOTS + LEAVES - 1
    for i in range(width):
        for part in range(rows // 8):
            at = (sub + 8 * part) * width + i
            chunk = at + shifts[0]
            for k in range(1, 8):
                chunk = jnp.where(at >= starts[k], at + shifts[k], chunk)
            first = (i * rows + 8 * part) * SLOTS
            chunks_vmem[pl.ds(first, 1024)] = jnp.where(at < total, chunk, null_chunk).reshape(1024)
    for part in range(rows // 8):
        group = sub + (8 * part + 1)
        following = jnp.where(target_of == LEAVES - 1, finished, target_of + 1)
        following = jnp.where(group * width < total, group * SLOTS + target_of, following)
        following = jnp.where(group > groups, finished, following)
        chunks_vmem[pl.ds((width * rows + 8 * part) * SLOTS, 1024)] = following.reshape(1024)
    to_scalars = pltpu.make_async_copy(chunks_vmem, chunks_smem, sem)
    to_scalars.start()

    unit = leaves // 2
    limb = lax.broadcasted_iota(jnp.int32, (16, 4 * SLOTS), 0)
    column = lax.broadcasted_iota(jnp.int32, (16, 4 * SLOTS), 1)
    gather = ((limb < 12) & ((limb & 3) == column // SLOTS)).astype(jnp.float32).astype(jnp.bfloat16)

    def limbs_of(tile):
        high = tile.astype(jnp.bfloat16).astype(jnp.float32)
        rest = tile - high
        middle = rest.astype(jnp.bfloat16).astype(jnp.float32)
        low = rest - middle
        return jnp.concatenate([high, middle, low, jnp.zeros((4, SLOTS), jnp.float32)], axis=0)

    value = lax.broadcasted_iota(jnp.int32, (4, SLOTS), 0)

    def spread_leaf(first, _):
        lhs = []
        for u in range(unit):
            tile = source_table[first * unit + u]
            tile = jnp.where(value == 3, jnp.maximum(tile, 0.0), tile)
            lhs.append(jnp.transpose(limbs_of(tile)).astype(jnp.bfloat16))
        copied = jnp.dot(jnp.concatenate(lhs, axis=0), gather, preferred_element_type=jnp.float32)
        pieces = unit * SLOTS // ROWS
        spread[pl.ds(first * pieces, pieces)] = copied.reshape(pieces, ROWS, 4 * SLOTS)
        return 0

    lax.fori_loop(0, leaves // unit, spread_leaf, 0)
    spread[null_chunk] = jnp.zeros((ROWS, 4 * SLOTS), jnp.float32)

    to_scalars.wait()

    def pull_on(target, chunks):
        centre = [jnp.broadcast_to(target_table[target, c : c + 1, :], (8, SLOTS)) for c in range(3)]
        pulls = None
        for chunk in chunks:
            for row in range(0, ROWS, 8):
                piece = [spread[chunk, row : row + 8, SLOTS * c : SLOTS * c + SLOTS] for c in range(4)]
                delta = [piece[c] - centre[c] for c in range(3)]
                squares = [d * d for d in delta]
                r = lax.rsqrt((squares[0] + softening) + (squares[1] + squares[2]))
                weight = (piece[3] * r) * (r * r)
                parts = [weight * d for d in delta]
                pulls = parts if pulls is None else [a + b for a, b in zip(pulls, parts)]
        for c in range(3):
            sums[target, 8 * c : 8 * c + 8, :] += pulls[c]

    def chunks_at(at):
        return tuple(chunks_smem[at + i * rows * SLOTS] for i in range(width))

    def body(state):
        at, chunks = state
        for _ in range(blocks):
            pull_on(at & (LEAVES - 1), chunks)
            at = chunks_smem[at + width * rows * SLOTS]
            chunks = chunks_at(at)
        return at, chunks

    zero = jnp.int32(0)
    lax.while_loop(lambda s: s[0] < finished, body, (zero, chunks_at(zero)))


def own_kernel(table, sources, out, slot_of, picked, spread, sums, chunks_vmem, chunks_smem, sem):
    ids = sources[...]
    ids = jnp.where(ids < LEAVES, ids, -1)
    clear_sums(sums)
    number_neighbours(sources, slot_of, picked)
    pair_forces(table, table, ids, spread, sums, chunks_vmem, chunks_smem, sem, LEAVES)

    def finish(i, _):
        for part in range(8):
            t = i * 8 + part
            for c in range(3):
                out[t, c : c + 1, :] = jnp.sum(sums[t, 8 * c : 8 * c + 8, :], axis=0, keepdims=True)
        return 0

    lax.fori_loop(0, LEAVES // 8, finish, 0)


def near_kernel(before, after, table, own_pull, sources, slot_of, picked_vmem, out, picked, picked_sem, leaves, spread, sums, chunks_vmem, chunks_smem, sem):
    to_scalars = pltpu.make_async_copy(picked_vmem, picked, picked_sem)
    to_scalars.start()
    clear_sums(sums)
    to_scalars.wait()

    def gather(i, _):
        for part in range(8):
            s = i * 8 + part
            leaves[s] = before[picked[0, s]]
            leaves[NEAR + s] = after[picked[0, NEAR + s]]
        return 0

    lax.fori_loop(0, NEAR // 8, gather, 0)
    ids = sources[...]
    within = ids & (LEAVES - 1)
    below = jnp.take_along_axis(slot_of[:, :LEAVES], within, axis=1)
    above = jnp.take_along_axis(slot_of[:, LEAVES:], within, axis=1)
    ids = jnp.where(ids < LEAVES, -1, jnp.where(ids < 2 * LEAVES, below, above))
    pair_forces(leaves, table, ids, spread, sums, chunks_vmem, chunks_smem, sem, 2 * NEAR)

    def finish(i, _):
        for part in range(8):
            t = i * 8 + part
            at = pl.multiple_of(t * SLOTS, SLOTS)
            living = table[t, 3:4, :] >= 0.0
            for c in range(3):
                pull = jnp.sum(sums[t, 8 * c : 8 * c + 8, :], axis=0, keepdims=True) + own_pull[t, c : c + 1, :]
                out[c : c + 1, pl.ds(at, SLOTS)] = jnp.where(living, pull, 0.0)
        return 0

    lax.fori_loop(0, LEAVES // 8, finish, 0)


def f32(*shape):
    return jax.ShapeDtypeStruct(shape, jnp.float32)


def i32(*shape):
    return jax.ShapeDtypeStruct(shape, jnp.int32)


vmem = pl.BlockSpec(memory_space=pltpu.VMEM)
smem = pl.BlockSpec(memory_space=pltpu.SMEM)


def pair_scratch(leaves):
    list_words = (width + 1) * (8 * SLOTS // ROWS // width + 8) * SLOTS
    return [
        pltpu.VMEM((leaves * (SLOTS // ROWS) + 1, ROWS, 4 * SLOTS), jnp.float32),
        pltpu.VMEM((LEAVES, 24, SLOTS), jnp.float32),
        pltpu.VMEM((list_words,), jnp.int32),
        pltpu.SMEM((list_words,), jnp.int32),
        pltpu.SemaphoreType.DMA,
    ]


def cost(us):
    return pl.CostEstimate(flops=int(us * 8_000_000), bytes_accessed=0, transcendentals=0)


def pack(positions, masses, counts):
    return pl.pallas_call(
        pack_kernel,
        out_shape=pltpu.VMEM((LEAVES, 4, SLOTS), jnp.float32),
        in_specs=[vmem, vmem, smem],
        out_specs=vmem,
        name="pack",
    )(positions, masses, counts)


def own_forces(table, sources):
    return pl.pallas_call(
        own_kernel,
        out_shape=(f32(LEAVES, 4, SLOTS), i32(8, 2 * LEAVES), i32(8, SLOTS)),
        in_specs=[vmem, vmem],
        out_specs=(vmem, vmem, vmem),
        scratch_shapes=pair_scratch(LEAVES),
        compiler_params=pltpu.CompilerParams(vmem_limit_bytes=42 * MIB),
        cost_estimate=cost(20),
        name="own_forces",
    )(table, sources)


def near_forces(before, after, table, own_pull, sources, slot_of, picked):
    return pl.pallas_call(
        near_kernel,
        out_shape=f32(3, LEAVES * SLOTS),
        in_specs=[vmem, vmem, vmem, vmem, vmem, vmem, vmem],
        out_specs=vmem,
        scratch_shapes=[
            pltpu.SMEM((8, SLOTS), jnp.int32),
            pltpu.SemaphoreType.DMA,
            pltpu.VMEM((2 * NEAR, 4, SLOTS), jnp.float32),
            *pair_scratch(2 * NEAR),
        ],
        compiler_params=pltpu.CompilerParams(vmem_limit_bytes=30 * MIB),
        cost_estimate=cost(12),
        name="near_forces",
    )(before, after, table, own_pull, sources, slot_of, picked)


def on_device(positions, masses, counts, sources):
    sources = sources.T
    sent = pack(positions, masses, counts)
    table = lax.all_to_all(sent, "col", split_axis=0, concat_axis=0, tiled=True)
    size = lax.axis_size("row")
    up = [(i, (i + 1) % size) for i in range(size)]
    down = [(j, i) for i, j in up]
    before = lax.ppermute(table, "row", up)
    after = lax.ppermute(table, "row", down)
    own_pull, slot_of, picked = own_forces(table, sources)
    return near_forces(before, after, table, own_pull, sources, slot_of, picked)


def solution(mesh):
    return jax.shard_map(
        on_device,
        mesh=mesh,
        in_specs=(
            P(None, ("row", "col")),
            P(None, ("row", "col")),
            P(None, ("row", "col")),
            P(("row", "col"), None),
        ),
        out_specs=P(None, ("row", "col")),
        check_vma=False,
    )
```

```python
import jax
import jax.numpy as jnp
from jax import lax
from jax.experimental import pallas as pl
from jax.experimental.pallas import tpu as pltpu
from jax.sharding import PartitionSpec as P

softening = 2.5e-07
SHIFT = 3
ROWS = 1 << SHIFT
width = 8
LEAVES = 128
SLOTS = 128
NEAR = 32
DEAD = -1.0
MIB = 1024 * 1024


def pack_kernel(positions, masses, counts, out):
    lane = lax.broadcasted_iota(jnp.int32, (1, SLOTS), 1)

    def group(first, _):
        for part in range(8):
            leaf = first * 8 + part
            at = pl.multiple_of(leaf * SLOTS, SLOTS)
            out[leaf, 0:3, :] = positions[:, pl.ds(at, SLOTS)]
            out[leaf, 3:4, :] = jnp.where(lane < counts[0, leaf], masses[:, pl.ds(at, SLOTS)], DEAD)
        return 0

    lax.fori_loop(0, LEAVES // 8, group, 0)


def number_neighbours(sources, slot_of, picked):
    low = lax.broadcasted_iota(jnp.int32, (2 * LEAVES, SLOTS), 0) + LEAVES
    named = jnp.zeros((2 * LEAVES, SLOTS), jnp.bool_)
    for k in range(8):
        named = named | (low == sources[k : k + 1, :])
    flags = named.astype(jnp.float32).astype(jnp.bfloat16)
    ones = jnp.ones((8, SLOTS), jnp.bfloat16)
    lanes = (((1,), (1,)), ((), ()))
    uses = lax.dot_general(ones, flags, lanes, preferred_element_type=jnp.float32)
    present = uses > 0.5
    row = lax.broadcasted_iota(jnp.int32, (2 * LEAVES, 2 * LEAVES), 0)
    col = lax.broadcasted_iota(jnp.int32, (2 * LEAVES, 2 * LEAVES), 1)
    before = (row < col).astype(jnp.float32).astype(jnp.bfloat16)
    ahead = present.astype(jnp.float32).astype(jnp.bfloat16)
    rank = lax.dot_general(ahead, before, (((1,), (0,)), ((), ())), preferred_element_type=jnp.float32)
    rank = rank.astype(jnp.int32)
    slot_of[...] = jnp.minimum(rank, 2 * NEAR - 1)
    slot = lax.broadcasted_iota(jnp.int32, (SLOTS, 2 * LEAVES), 0)
    chosen = (slot == jnp.where(present, rank, -1)[0:1, :]).astype(jnp.float32).astype(jnp.bfloat16)
    leaf = lax.broadcasted_iota(jnp.int32, (8, 2 * LEAVES), 1) & (LEAVES - 1)
    leaf = leaf.astype(jnp.float32).astype(jnp.bfloat16)
    picked[...] = lax.dot_general(leaf, chosen, lanes, preferred_element_type=jnp.float32).astype(jnp.int32)


def clear_sums(sums):
    def clear(i, _):
        for part in range(8):
            sums[i * 8 + part] = jnp.zeros((24, SLOTS), jnp.float32)
        return 0

    lax.fori_loop(0, LEAVES // 8, clear, 0)


def pair_forces(source_table, target_table, ids, spread, sums, chunks_vmem, chunks_smem, sem, leaves):
    per_leaf = SLOTS // ROWS
    most = 8 * per_leaf
    null_chunk = leaves * per_leaf
    ones = jnp.ones((8, SLOTS), jnp.bfloat16)
    live = (source_table[:, 3, :] >= 0.0).astype(jnp.float32).astype(jnp.bfloat16)
    if leaves < SLOTS:
        live = jnp.concatenate([live, jnp.zeros((SLOTS - leaves, SLOTS), jnp.bfloat16)], axis=0)
    count = lax.dot_general(ones, live, (((1,), (1,)), ((), ())), preferred_element_type=jnp.float32)
    size = (count.astype(jnp.int32) + (ROWS - 1)) >> SHIFT
    mine = ids >= 0
    leaf = jnp.where(mine, ids, 0)
    size = jnp.where(mine, jnp.take_along_axis(size, leaf, axis=1), 0)
    sub = lax.broadcasted_iota(jnp.int32, (8, SLOTS), 0)
    starts, shifts, total = [], [], jnp.zeros((8, SLOTS), jnp.int32)
    for k in range(8):
        starts.append(total)
        shifts.append(jnp.broadcast_to(leaf[k : k + 1, :], (8, SLOTS)) * per_leaf - total)
        total = total + jnp.broadcast_to(size[k : k + 1, :], (8, SLOTS))
    groups = most // width
    rows = groups + 8
    target_of = lax.broadcasted_iota(jnp.int32, (8, SLOTS), 1)
    finished = groups * SLOTS + LEAVES - 1
    for i in range(width):
        for part in range(rows // 8):
            at = (sub + 8 * part) * width + i
            chunk = at + shifts[0]
            for k in range(1, 8):
                chunk = jnp.where(at >= starts[k], at + shifts[k], chunk)
            first = (i * rows + 8 * part) * SLOTS
            chunks_vmem[pl.ds(first, 1024)] = jnp.where(at < total, chunk, null_chunk).reshape(1024)
    for part in range(rows // 8):
        group = sub + (8 * part + 1)
        following = jnp.where(target_of == LEAVES - 1, finished, target_of + 1)
        following = jnp.where(group * width < total, group * SLOTS + target_of, following)
        following = jnp.where(group > groups, finished, following)
        chunks_vmem[pl.ds((width * rows + 8 * part) * SLOTS, 1024)] = following.reshape(1024)
    to_scalars = pltpu.make_async_copy(chunks_vmem, chunks_smem, sem)
    to_scalars.start()

    unit = leaves // 2
    limb = lax.broadcasted_iota(jnp.int32, (16, 4 * SLOTS), 0)
    column = lax.broadcasted_iota(jnp.int32, (16, 4 * SLOTS), 1)
    gather = ((limb < 12) & ((limb & 3) == column // SLOTS)).astype(jnp.float32).astype(jnp.bfloat16)

    def limbs_of(tile):
        high = tile.astype(jnp.bfloat16).astype(jnp.float32)
        rest = tile - high
        middle = rest.astype(jnp.bfloat16).astype(jnp.float32)
        low = rest - middle
        return jnp.concatenate([high, middle, low, jnp.zeros((4, SLOTS), jnp.float32)], axis=0)

    value = lax.broadcasted_iota(jnp.int32, (4, SLOTS), 0)

    def spread_leaf(first, _):
        lhs = []
        for u in range(unit):
            tile = source_table[first * unit + u]
            tile = jnp.where(value == 3, jnp.maximum(tile, 0.0), tile)
            lhs.append(jnp.transpose(limbs_of(tile)).astype(jnp.bfloat16))
        copied = jnp.dot(jnp.concatenate(lhs, axis=0), gather, preferred_element_type=jnp.float32)
        pieces = unit * SLOTS // ROWS
        spread[pl.ds(first * pieces, pieces)] = copied.reshape(pieces, ROWS, 4 * SLOTS)
        return 0

    lax.fori_loop(0, leaves // unit, spread_leaf, 0)
    spread[null_chunk] = jnp.zeros((ROWS, 4 * SLOTS), jnp.float32)

    to_scalars.wait()

    def pull_on(target, chunks):
        centre = [jnp.broadcast_to(target_table[target, c : c + 1, :], (8, SLOTS)) for c in range(3)]
        pulls = None
        for chunk in chunks:
            for row in range(0, ROWS, 8):
                piece = [spread[chunk, row : row + 8, SLOTS * c : SLOTS * c + SLOTS] for c in range(4)]
                delta = [piece[c] - centre[c] for c in range(3)]
                squares = [d * d for d in delta]
                r = lax.rsqrt((squares[0] + softening) + (squares[1] + squares[2]))
                weight = (piece[3] * r) * (r * r)
                parts = [weight * d for d in delta]
                pulls = parts if pulls is None else [a + b for a, b in zip(pulls, parts)]
        for c in range(3):
            sums[target, 8 * c : 8 * c + 8, :] += pulls[c]

    def chunks_at(at):
        return tuple(chunks_smem[at + i * rows * SLOTS] for i in range(width))

    def body(state):
        at, chunks = state
        for _ in range(32 if leaves == LEAVES else 20):
            pull_on(at & (LEAVES - 1), chunks)
            at = chunks_smem[at + width * rows * SLOTS]
            chunks = chunks_at(at)
        return at, chunks

    zero = jnp.int32(0)
    lax.while_loop(lambda s: s[0] < finished, body, (zero, chunks_at(zero)))


def own_kernel(table, sources, out, slot_of, picked, spread, sums, chunks_vmem, chunks_smem, sem):
    ids = sources[...]
    ids = jnp.where(ids < LEAVES, ids, -1)
    clear_sums(sums)
    number_neighbours(sources, slot_of, picked)
    pair_forces(table, table, ids, spread, sums, chunks_vmem, chunks_smem, sem, LEAVES)

    def finish(i, _):
        for part in range(8):
            t = i * 8 + part
            for c in range(3):
                out[t, c : c + 1, :] = jnp.sum(sums[t, 8 * c : 8 * c + 8, :], axis=0, keepdims=True)
        return 0

    lax.fori_loop(0, LEAVES // 8, finish, 0)


def near_kernel(before, after, table, own_pull, sources, slot_of, picked_vmem, out, picked, picked_sem, leaves, spread, sums, chunks_vmem, chunks_smem, sem):
    to_scalars = pltpu.make_async_copy(picked_vmem, picked, picked_sem)
    to_scalars.start()
    clear_sums(sums)
    to_scalars.wait()

    def gather(i, _):
        for part in range(8):
            s = i * 8 + part
            leaves[s] = before[picked[0, s]]
            leaves[NEAR + s] = after[picked[0, NEAR + s]]
        return 0

    lax.fori_loop(0, NEAR // 8, gather, 0)
    ids = sources[...]
    within = ids & (LEAVES - 1)
    below = jnp.take_along_axis(slot_of[:, :LEAVES], within, axis=1)
    above = jnp.take_along_axis(slot_of[:, LEAVES:], within, axis=1)
    ids = jnp.where(ids < LEAVES, -1, jnp.where(ids < 2 * LEAVES, below, above))
    pair_forces(leaves, table, ids, spread, sums, chunks_vmem, chunks_smem, sem, 2 * NEAR)

    def finish(i, _):
        for part in range(8):
            t = i * 8 + part
            at = pl.multiple_of(t * SLOTS, SLOTS)
            living = table[t, 3:4, :] >= 0.0
            for c in range(3):
                pull = jnp.sum(sums[t, 8 * c : 8 * c + 8, :], axis=0, keepdims=True) + own_pull[t, c : c + 1, :]
                out[c : c + 1, pl.ds(at, SLOTS)] = jnp.where(living, pull, 0.0)
        return 0

    lax.fori_loop(0, LEAVES // 8, finish, 0)


def f32(*shape):
    return jax.ShapeDtypeStruct(shape, jnp.float32)


def i32(*shape):
    return jax.ShapeDtypeStruct(shape, jnp.int32)


vmem = pl.BlockSpec(memory_space=pltpu.VMEM)
smem = pl.BlockSpec(memory_space=pltpu.SMEM)


def pair_scratch(leaves):
    list_words = (width + 1) * (8 * SLOTS // ROWS // width + 8) * SLOTS
    return [
        pltpu.VMEM((leaves * (SLOTS // ROWS) + 1, ROWS, 4 * SLOTS), jnp.float32),
        pltpu.VMEM((LEAVES, 24, SLOTS), jnp.float32),
        pltpu.VMEM((list_words,), jnp.int32),
        pltpu.SMEM((list_words,), jnp.int32),
        pltpu.SemaphoreType.DMA,
    ]


def cost(us):
    return pl.CostEstimate(flops=int(us * 8_000_000), bytes_accessed=0, transcendentals=0)


def pack(positions, masses, counts):
    return pl.pallas_call(
        pack_kernel,
        out_shape=pltpu.VMEM((LEAVES, 4, SLOTS), jnp.float32),
        in_specs=[vmem, vmem, smem],
        out_specs=vmem,
        name="pack",
    )(positions, masses, counts)


def own_forces(table, sources):
    return pl.pallas_call(
        own_kernel,
        out_shape=(f32(LEAVES, 4, SLOTS), i32(8, 2 * LEAVES), i32(8, SLOTS)),
        in_specs=[vmem, vmem],
        out_specs=(vmem, vmem, vmem),
        scratch_shapes=pair_scratch(LEAVES),
        compiler_params=pltpu.CompilerParams(vmem_limit_bytes=42 * MIB),
        cost_estimate=cost(20),
        name="own_forces",
    )(table, sources)


def near_forces(before, after, table, own_pull, sources, slot_of, picked):
    return pl.pallas_call(
        near_kernel,
        out_shape=f32(3, LEAVES * SLOTS),
        in_specs=[vmem, vmem, vmem, vmem, vmem, vmem, vmem],
        out_specs=vmem,
        scratch_shapes=[
            pltpu.SMEM((8, SLOTS), jnp.int32),
            pltpu.SemaphoreType.DMA,
            pltpu.VMEM((2 * NEAR, 4, SLOTS), jnp.float32),
            *pair_scratch(2 * NEAR),
        ],
        compiler_params=pltpu.CompilerParams(vmem_limit_bytes=30 * MIB),
        cost_estimate=cost(12),
        name="near_forces",
    )(before, after, table, own_pull, sources, slot_of, picked)


def on_device(positions, masses, counts, sources):
    sources = sources.T
    sent = pack(positions, masses, counts)
    table = lax.all_to_all(sent, "col", split_axis=0, concat_axis=0, tiled=True)
    size = lax.axis_size("row")
    up = [(i, (i + 1) % size) for i in range(size)]
    down = [(j, i) for i, j in up]
    before = lax.ppermute(table, "row", up)
    after = lax.ppermute(table, "row", down)
    own_pull, slot_of, picked = own_forces(table, sources)
    return near_forces(before, after, table, own_pull, sources, slot_of, picked)


def solution(mesh):
    return jax.shard_map(
        on_device,
        mesh=mesh,
        in_specs=(
            P(None, ("row", "col")),
            P(None, ("row", "col")),
            P(None, ("row", "col")),
            P(("row", "col"), None),
        ),
        out_specs=P(None, ("row", "col")),
        check_vma=False,
    )
```
